1024 devices in a mesh: win: 64 (over y, z_hi, core), seq: 16 (over x, z_lo).
Axes of the slice: x: 8, y: 8, z: 8 (z_hi: 4, z_lo: 2; z = z_hi * 2 + z_lo), core: 2. Of those that a mesh axis runs over, the one named last changes fastest.
Arguments:
- qkv_grid: bfloat16 [90, 64, 32, 4608], P(None, 'win', 'seq'), may hold values from -160 to 160
- tokens: bfloat16 [90, 64, 32, 1536], P(None, 'win', 'seq'), may hold values from -6 to 6
- out_weight: bfloat16 [1536, 1536], replicated, may hold values from -0.625 to 0.625
- regions: int32 [90, 64, 32], P(None, 'win'), may hold values from 0 to 2, as said below
Outputs:
- mixed: bfloat16 [90, 64, 32, 1536], P(None, 'win', 'seq')
The draws below stay inside these ranges and needn't reach their ends.
Inputs may be any that keep to these rules, and one draw needn't show every extreme that they name: `regions`: columns 2m and 2m+1 of a window always have the same region id.
All inputs are finite; a program needn't handle non-finite values.
Results may differ from the reference program's by a relative error of at most 0.01.
Values may be sent and summed in bfloat16 or wider, within the bound.
No kernel may reach another device: no remote copies, remote signals or barrier semaphores. Data moves between devices by JAX's collectives and lax.ppermute only.
A program may use at most 32 MiB of HBM per device.

```python
import jax
import jax.numpy as jnp
from jax import lax

D = 1536
HEADS = 16
HD = 96
WH = 30
WW = 32
LATW = 3
REGIONS = 3
LAT = 90
LONWIN = 64


def draw_regions(key, part):
    region_pairs = jax.random.randint(jax.random.fold_in(key, 11), (LAT, LONWIN, WW // 2), 0, REGIONS)
    return jnp.repeat(region_pairs, 2, axis=2).astype(jnp.int32)


def draw_qkv_grid(key, part):
    columns = LONWIN * WW
    base = jax.random.normal(jax.random.fold_in(key, 21), (LAT, columns, 3, HEADS, HD), jnp.float32)
    base = jnp.clip(base, -6.0, 6.0)
    grid = jnp.roll(base, (WH // 2, WW // 2), (0, 1))
    return grid.reshape(LAT, LONWIN, WW, 3 * D).astype(jnp.bfloat16)


def block_scale(rng, extent, pieces, smallest, high):
    def one(dim, parts):
        heights = jax.random.uniform(jax.random.fold_in(jax.random.fold_in(rng, 6), dim), (parts,), jnp.float32, smallest / len(pieces), high / len(pieces))
        return jnp.repeat(jnp.exp(heights), extent[dim] // parts).reshape((-1,) + (1,) * (len(extent) - dim - 1))

    loudness = one(*pieces[0])
    for cut in pieces[1:]:
        loudness = loudness * one(*cut)
    return loudness


def normal_values(rng, dims, spread, most, cuts=(), dtype=jnp.bfloat16):
    drawn = jax.random.normal(rng, dims, jnp.float32) * spread
    if len(cuts) > 0:
        drawn = block_scale(rng, dims, cuts, -0.22, 0.18) * drawn
    return jnp.clip(drawn, min=-most, max=most).astype(dtype)


def setup_inputs(seed: int = 0) -> dict:
    key_list = jax.random.split(jax.random.key(seed), 5)
    qkv_grid = draw_qkv_grid(jax.random.fold_in(key_list[4], 71), 0)
    tokens = normal_values(key_list[1], (LAT, LONWIN, WW, D), 1.0, 6.0, ((1, 64), (2, 16)))
    out_weight = normal_values(key_list[2], (D, D), (D // 16) ** -0.5, 0.625)
    regions = draw_regions(jax.random.fold_in(key_list[4], 71), 0)
    return {"qkv_grid": qkv_grid, "tokens": tokens, "out_weight": out_weight, "regions": regions}


def attend(window_block, labels):
    queries = window_block[:, 0].astype(jnp.float32)
    key_rows = window_block[:, 1].astype(jnp.float32)
    values = window_block[:, 2].astype(jnp.float32)
    scores = jnp.einsum("qhd,khd->hqk", queries, key_rows) * (HD ** -0.5)
    allowed = labels[:, None] == labels[None, :]
    scores = jnp.where(allowed[None], scores, -1e30)
    largest = jnp.max(scores, axis=-1, keepdims=True)
    weights = jnp.exp(scores - largest)
    soft_weights = (weights / jnp.sum(weights, axis=-1, keepdims=True)).astype(jnp.bfloat16)
    result = jnp.einsum("hqk,khd->qhd", soft_weights.astype(jnp.float32), values)
    return result.astype(jnp.bfloat16)


def one_window(paired):
    return attend(paired[0], paired[1])


def reference(qkv_grid, tokens, out_weight, regions):
    columns = LONWIN * WW
    grid = qkv_grid.reshape(LAT, columns, 3, HEADS, HD)
    shifted = jnp.roll(grid, (-(WH // 2), -(WW // 2)), (0, 1))
    blocks = shifted.reshape(LATW, WH, LONWIN, WW, 3, HEADS, HD).transpose(0, 2, 1, 3, 4, 5, 6)
    blocks = blocks.reshape(LATW * LONWIN, WH * WW, 3, HEADS, HD)
    labels = regions.reshape(LATW, WH, LONWIN, WW).transpose(0, 2, 1, 3).reshape(LATW * LONWIN, WH * WW)
    attended = lax.map(one_window, (blocks, labels))
    attended = attended.reshape(LATW, LONWIN, WH, WW, D).transpose(0, 2, 1, 3, 4).reshape(LAT, columns, D)
    restored = jnp.roll(attended, (WH // 2, WW // 2), (0, 1))
    projected = jnp.dot(restored.reshape(LAT * columns, D), out_weight, preferred_element_type=jnp.float32)
    total = projected + tokens.reshape(LAT * columns, D).astype(jnp.float32)
    return total.astype(jnp.bfloat16).reshape(LAT, LONWIN, WW, D)
```

```python
import jax
import jax.numpy as jnp
from jax import lax
from jax.experimental import pallas as pl
from jax.experimental.pallas import tpu as pltpu
from jax.sharding import PartitionSpec as P

D = 1536
HEADS = 16
HD = 96
WH = 30
WW = 32
BANDS = 3
ROWS = 64
PACK = 144
PIECE = 48
KEYS = HEADS * ROWS
HIDE = -1e30


def lane_block(rows):
    return lax.broadcasted_iota(jnp.int32, (rows, 128), 1) // 32


def head_lanes(load, h):
    g, j = divmod(h, 4)
    if j == 0:
        return load(3 * g)
    if j == 3:
        return load(3 * g + 2)
    first, second = load(3 * g + j - 1), load(3 * g + j)
    block = lane_block(first.shape[0])
    return jnp.where(block < 3 - j, second, first)


def pack_rows(load, h):
    tail = head_lanes(lambda t: load(t, PACK, PIECE), h).astype(jnp.float32)
    out = []
    for i in range(3):
        rows = head_lanes(lambda t: load(t, PIECE * i, PIECE), h)
        moved = pltpu.roll(tail, 32 * (3 - i), 1).astype(jnp.bfloat16)
        out.append(jnp.where(lane_block(PIECE) == 3 - h % 4, moved, rows))
    return out


def pack_in_kernel(x_ref, o_ref, flat):
    for b in range(BANDS):
        flat[ROWS * (b + 1) - 4:ROWS * (b + 1), :] = jnp.zeros((4, 3 * D), jnp.bfloat16)
    for dst, src, count in SPANS:
        for r in range(0, count, 8):
            n = min(8, count - r)
            start = 2 * (dst + r)
            flat[start:start + 2 * n, :] = x_ref[src + r:src + r + n, 0].reshape(2 * n, 3 * D)
    for t in range(3):
        for h in range(HEADS):
            def load(tile, start, size):
                lanes = (12 * t + tile) * 128
                return flat[start:start + size, lanes:lanes + 128]
            for i, rows in enumerate(pack_rows(load, h)):
                start = PACK * t + PIECE * i
                o_ref[h, start:start + PIECE, :] = rows


SPANS = ((0, 15, 30), (32, 45, 30), (64, 75, 15), (79, 0, 15))


def pack_qkv(x):
    return pl.pallas_call(
        pack_in_kernel,
        out_shape=jax.ShapeDtypeStruct((HEADS, 3 * PACK, 128), jnp.bfloat16),
        in_specs=[pl.BlockSpec(memory_space=pltpu.VMEM)],
        out_specs=pl.BlockSpec(memory_space=pltpu.VMEM),
        scratch_shapes=[pltpu.VMEM((BANDS * ROWS, 3 * D), jnp.bfloat16)],
        cost_estimate=pl.CostEstimate(flops=10**7, bytes_accessed=4 * 10**6, transcendentals=0),
        name="pack_qkv",
    )(x)


def attend_kernel(head_ref, x_ref, labels_ref, o_ref, q_s, k_s, v_s, r_s):
    junk = 3 - lax.rem(head_ref[0], 4)
    start = lax.rem(junk + 1, 4)
    f32, bf16 = jnp.float32, jnp.bfloat16
    scale = HD ** -0.5 * 1.4426950408889634

    def turned(x, shift):
        return pltpu.roll(x.astype(f32), shift, 1).astype(bf16)

    def tail_rows(rows):
        block = lane_block(PIECE)
        a, b, c = (turned(rows(i), 32 * (i + 1)) for i in range(3))
        second = lax.rem(start + 1, 4)
        return jnp.where(block == start, a, jnp.where(block == second, b, c))

    columns = labels_ref[...].astype(bf16)
    picks = (lax.broadcasted_iota(jnp.int32, (WW, HEADS * 128), 0)
             == 2 * (lax.broadcasted_iota(jnp.int32, (WW, HEADS * 128), 1) // 128))
    picks = picks.astype(bf16)
    lane = lax.broadcasted_iota(jnp.int32, (ROWS, 128), 1)
    region = lane - 32 * junk
    inside = (region >= 0) & (region < 32)
    for b in range(BANDS):
        token = lax.broadcasted_iota(jnp.int32, (ROWS, 90), 0)
        grows = (token // 2 + WH * b == lax.broadcasted_iota(jnp.int32, (ROWS, 90), 1)) & (token < 60)
        by_column = lax.dot_general(
            grows.astype(bf16), columns, (((1,), (1,)), ((), ())), preferred_element_type=f32)
        r_s[...] = jnp.dot(by_column.astype(bf16), picks, preferred_element_type=f32)
        pad = lax.broadcasted_iota(jnp.int32, (ROWS, 128), 0) >= 60
        for p in range(HEADS):
            label = jnp.where(pad, 3, r_s[:, 128 * p:128 * (p + 1)].astype(jnp.int32))
            same = label == region
            rows = []
            for t in range(3):
                if b < 2:
                    rows.append(x_ref[p, PACK * t + ROWS * b:PACK * t + ROWS * (b + 1), :])
                else:
                    head = x_ref[p, PACK * t + 2 * ROWS:PACK * (t + 1), :]
                    tail = tail_rows(lambda i: x_ref[p, PACK * t + PIECE * i:PACK * t + PIECE * (i + 1), :])
                    rows.append(jnp.concatenate([head, tail], 0))
            here = slice(ROWS * p, ROWS * (p + 1))
            q_s[here, :] = jnp.where(inside, jnp.where(same, 1.0, 0.0).astype(bf16), rows[0])
            k_s[here, :] = jnp.where(inside, jnp.where(same, 0.0, HIDE).astype(bf16), rows[1])
            v_s[here, :128] = rows[2]
        v_s[:, 128:] = jnp.ones((KEYS, 128), bf16)
        block_rows = 256
        for n in range(KEYS // block_rows):
            q = q_s[block_rows * n:block_rows * (n + 1), :]
            s = lax.dot_general(q, k_s[...], (((1,), (1,)), ((), ())), preferred_element_type=f32)
            m = jnp.max(s, axis=1, keepdims=True)
            weights = jnp.exp2((s - m) * scale).astype(bf16)
            acc = jnp.dot(weights, v_s[...], preferred_element_type=f32)
            out = (acc[:, :128] / acc[:, 128:]).astype(bf16)
            for p4 in range(block_rows // ROWS):
                p = n * (block_rows // ROWS) + p4
                mine = out[ROWS * p4:ROWS * (p4 + 1), :]
                if b < 2:
                    o_ref[p, ROWS * b:ROWS * (b + 1), :] = mine
                else:
                    o_ref[p, 2 * ROWS:PACK, :] = mine[:PACK - 2 * ROWS]
                    tail = mine[PACK - 2 * ROWS:]
                    unused = lane_block(PIECE) == junk
                    for i in range(3):
                        rows = slice(PIECE * i, PIECE * (i + 1))
                        o_ref[p, rows, :] = jnp.where(unused, turned(tail, 32 * (3 - i)), o_ref[p, rows, :])


def attend(head, packed, labels):
    vmem = pl.BlockSpec(memory_space=pltpu.VMEM)
    return pl.pallas_call(
        attend_kernel,
        out_shape=jax.ShapeDtypeStruct((HEADS, PACK, 128), jnp.bfloat16),
        in_specs=[pl.BlockSpec(memory_space=pltpu.SMEM), vmem, vmem],
        out_specs=vmem,
        scratch_shapes=[
            pltpu.VMEM((KEYS, 128), jnp.bfloat16),
            pltpu.VMEM((KEYS, 128), jnp.bfloat16),
            pltpu.VMEM((KEYS, 256), jnp.bfloat16),
            pltpu.VMEM((ROWS, HEADS * 128), jnp.float32),
        ],
        cost_estimate=pl.CostEstimate(flops=3 * 4 * KEYS * KEYS * 128, bytes_accessed=3 * 10**6, transcendentals=3 * KEYS * KEYS),
        name="attend",
    )(head, packed, labels)


def project_kernel(x_ref, tokens_ref, weight_ref, o_ref, a_s):
    f32, bf16 = jnp.float32, jnp.bfloat16
    block = lane_block(PIECE)

    def turned(x, shift):
        return pltpu.roll(x.astype(f32), shift, 1).astype(bf16)

    def tail(h):
        first = (3 * h) % 4
        a, b, c = (turned(x_ref[h, PIECE * i:PIECE * (i + 1), :], 32 * (i + 1)) for i in range(3))
        return jnp.where(block == first, a, jnp.where(block == (first + 1) % 4, b, c))

    for g in range(HEADS // 4):
        for part in range(4):
            if part < 3:
                rows = [x_ref[4 * g + j, PIECE * part:PIECE * (part + 1), :] for j in range(4)]
            else:
                rows = [tail(4 * g + j) for j in range(4)]
            for i in range(3):
                a_s[PIECE * part:PIECE * (part + 1), 128 * (3 * g + i):128 * (3 * g + i + 1)] = jnp.where(
                    block < 3 - i, rows[i], rows[i + 1])
    for n in range(D // 512):
        cols = slice(512 * n, 512 * (n + 1))
        total = jnp.dot(a_s[...], weight_ref[:, cols], preferred_element_type=f32)
        for dst, src, count in SPANS:
            part = total[2 * dst:2 * (dst + count)].reshape(count, 2, 512)
            here = (slice(src, src + count), 0, slice(None), cols)
            o_ref[here] = (part + tokens_ref[here].astype(f32)).astype(bf16)


def project(returned, tokens, weight):
    vmem = pl.BlockSpec(memory_space=pltpu.VMEM)
    return pl.pallas_call(
        project_kernel,
        out_shape=jax.ShapeDtypeStruct(tokens.shape, jnp.bfloat16),
        in_specs=[vmem] * 3,
        out_specs=vmem,
        scratch_shapes=[pltpu.VMEM((BANDS * ROWS, D), jnp.bfloat16)],
        cost_estimate=pl.CostEstimate(flops=2 * 192 * D * D, bytes_accessed=7 * 10**6, transcendentals=0),
        name="project",
    )(returned, tokens, weight)


def per_device(qkv_grid, tokens, out_weight, regions):
    windows, members = lax.axis_size("win"), lax.axis_size("seq")
    half = members // 2
    groups = [
        [w * members + half + i for i in range(half)] + [(w + 1) % windows * members + i for i in range(half)]
        for w in range(windows)
    ]

    def exchange(x):
        return lax.all_to_all(x, ("win", "seq"), 0, 0, axis_index_groups=groups, tiled=True)

    seat = lax.axis_index("seq")
    labels = regions[:, 0].T
    western = lax.ppermute(labels, "win", [(w, (w + 1) % windows) for w in range(windows)])
    labels = jnp.where(seat < half, western, labels)
    head = lax.rem(seat + half, members).reshape(1)
    received = exchange(pack_qkv(qkv_grid))
    returned = exchange(attend(head, received, labels))
    return project(returned, tokens, out_weight)


def solution(mesh):
    in_specs = (P(None, "win", "seq", None), P(None, "win", "seq", None), P(), P(None, "win", None))
    out_specs = P(None, "win", "seq", None)
    return jax.shard_map(
        per_device, mesh=mesh, in_specs=in_specs, out_specs=out_specs, check_vma=False
    )
```

```python
import jax
import jax.numpy as jnp
from jax import lax
from jax.experimental import pallas as pl
from jax.experimental.pallas import tpu as pltpu
from jax.sharding import PartitionSpec as P

D = 1536
HEADS = 16
HD = 96
WH = 30
WW = 32
BANDS = 3
ROWS = 64
TOKENS = 184
SENT = 416
TAIL = 136
PACK = 144
PIECE = 48
REST = 40
KEYS = HEADS * ROWS
HIDE = -1e30


def lane_block(rows):
    return lax.broadcasted_iota(jnp.int32, (rows, 128), 1) // 32


def head_lanes(load, h):
    g, j = divmod(h, 4)
    if j == 0:
        return load(3 * g)
    if j == 3:
        return load(3 * g + 2)
    first, second = load(3 * g + j - 1), load(3 * g + j)
    block = lane_block(first.shape[0])
    return jnp.where(block < 3 - j, second, first)


def turned(x, shift):
    return pltpu.roll(x.astype(jnp.float32), shift, 1).astype(jnp.bfloat16)


SPANS = ((0, 15, 30), (30, 75, 2), (32, 45, 30), (62, 77, 13), (75, 0, 15))
SEGMENTS = ((0, 136, 0, 0, 0, 0), (136, 184, 0, 136, 1, 0), (184, 272, 1, 0, 1, 48), (272, 368, 1, 88, 2, 0), (368, 408, 2, 0, 2, 96))


def pack_kernel(seat_ref, x_ref, labels_ref, o_ref, flat):
    f32, bf16 = jnp.float32, jnp.bfloat16
    flat[TOKENS - 8:, :] = jnp.zeros((flat.shape[0] - TOKENS + 8, 3 * D), bf16)
    for dst, src, count in SPANS:
        for r in range(0, count, 8):
            n = min(8, count - r)
            start = 2 * (dst + r)
            flat[start:start + 2 * n, :] = x_ref[src + r:src + r + n, 0].reshape(2 * n, 3 * D)
    row = lax.broadcasted_iota(jnp.int32, (8, WW), 0)
    column = lax.rem(2 * seat_ref[0] + jnp.where(row < 3, 0, WW // 2), WW)
    picks = (lax.broadcasted_iota(jnp.int32, (8, WW), 1) == column).astype(bf16)
    picked = jnp.dot(picks, labels_ref[...].astype(bf16), preferred_element_type=f32).astype(bf16)
    grid_row = lax.broadcasted_iota(jnp.int32, (90, 128), 0)
    lane = lax.broadcasted_iota(jnp.int32, (90, 128), 1) % 32
    band = lax.broadcasted_iota(jnp.int32, (8, 128), 0) % 3
    labels = jnp.zeros((8, 128), f32)
    for b in range(BANDS):
        place = ((grid_row == lane + WH * b) & (lane < WH)).astype(bf16)
        labels += jnp.where(band == b, jnp.dot(picked, place, preferred_element_type=f32), 0.0)
    labels = labels.astype(bf16)
    for h in range(HEADS):
        def rows(t, start, size):
            def load(tile):
                lanes = (12 * t + tile) * 128
                return flat[start:start + size, lanes:lanes + 128]
            return head_lanes(load, h)
        tail = rows(2, TOKENS - TAIL, TAIL)
        for start, end, t, first, section, skip in SEGMENTS:
            size = end - start
            moved = turned(tail[skip:skip + size], 32 * (3 - section))
            o_ref[h, start:end, :] = jnp.where(lane_block(size) == 3 - h % 4, moved, rows(t, first, size))
        o_ref[h, SENT - 8:, :] = jnp.where(lane_block(8) == 3 - h % 4, labels, rows(2, 40, 8))


def pack_qkv(seat, x, labels):
    vmem = pl.BlockSpec(memory_space=pltpu.VMEM)
    return pl.pallas_call(
        pack_kernel,
        out_shape=jax.ShapeDtypeStruct((HEADS, SENT, 128), jnp.bfloat16),
        in_specs=[pl.BlockSpec(memory_space=pltpu.SMEM), vmem, vmem],
        out_specs=vmem,
        scratch_shapes=[pltpu.VMEM((192, 3 * D), jnp.bfloat16)],
        cost_estimate=pl.CostEstimate(flops=10**7, bytes_accessed=4 * 10**6, transcendentals=0),
        compiler_params=pltpu.CompilerParams(vmem_limit_bytes=12 * 2**20),
        name="pack_qkv",
    )(seat, x, labels)


def attend_kernel(seat_ref, x_ref, o_ref, q_s, k_s, v_s, t_s, r_s):
    junk = 3 - lax.rem(seat_ref[0], 4)
    first = lax.rem(junk + 1, 4)
    second = lax.rem(junk + 2, 4)
    f32, bf16 = jnp.float32, jnp.bfloat16
    i32 = jnp.int32
    scale = HD ** -0.5 * 1.4426950408889634

    lane = lax.broadcasted_iota(i32, (ROWS, 128), 1) - 32 * junk
    inside = (lane >= 0) & (lane < 32)
    row = lax.broadcasted_iota(i32, (ROWS, 128), 0)
    sent_labels = jnp.concatenate([x_ref[p, SENT - 8:, :] for p in range(HEADS // 2)], 0)
    pick_row = lax.broadcasted_iota(i32, (ROWS, HEADS * 128), 0)
    pick_source = lax.broadcasted_iota(i32, (ROWS, HEADS * 128), 1) // 128
    pick_base = 8 * (pick_source % 8) + 3 * (pick_source // 8)
    tail_block = lane_block(TAIL)
    rest_block = lane_block(REST)
    eight = lax.broadcasted_iota(i32, (8, 128), 0)

    def block_of(load, b):
        if b < 2:
            return load(ROWS * b, ROWS)
        last = jnp.where(eight < 4, load(TOKENS - 8, 8), load(56, 8))
        return jnp.concatenate([load(120, 56), last], 0)

    for b in range(BANDS):
        token = jnp.where(row < 60, row, row - 60) if b == 2 else row
        spare = (row < 4) if b == 2 else (row >= 60)
        grows = (inside & (lane == token // 2)).astype(bf16)
        by_source = lax.dot_general(
            grows, sent_labels, (((1,), (1,)), ((), ())), preferred_element_type=f32).astype(bf16)
        picks = (pick_row == pick_base + b).astype(bf16)
        r_s[...] = jnp.dot(by_source, picks, preferred_element_type=f32)
        for p in range(HEADS):
            label = jnp.where(spare, 3, r_s[:, 128 * p:128 * (p + 1)].astype(i32))
            same = label == lane
            q = block_of(lambda start, size: x_ref[p, start:start + size, :], b)
            k = block_of(lambda start, size: x_ref[p, TOKENS + start:TOKENS + start + size, :], b)
            here = slice(ROWS * p, ROWS * (p + 1))
            q_s[here, :] = jnp.where(inside, jnp.where(same, 1.0, 0.0).astype(bf16), q)
            k_s[here, :] = jnp.where(inside, jnp.where(same, 0.0, HIDE).astype(bf16), k)
            if b == 0:
                x, y, z = (turned(x_ref[p, TAIL * i:TAIL * (i + 1), :], 32 * (i + 1)) for i in range(3))
                t_s[p, :TOKENS - TAIL, :] = x_ref[p, 2 * TOKENS:3 * TOKENS - TAIL, :]
                t_s[p, TOKENS - TAIL:, :] = jnp.where(tail_block == first, x, jnp.where(tail_block == second, y, z))
            v_s[here, :128] = block_of(lambda start, size: t_s[p, start:start + size, :], b)
        if b == 0:
            v_s[:, 128:] = jnp.ones((KEYS, 128), bf16)
        block_rows = 256
        for n in range(KEYS // block_rows):
            q = q_s[block_rows * n:block_rows * (n + 1), :]
            s = lax.dot_general(q, k_s[...], (((1,), (1,)), ((), ())), preferred_element_type=f32)
            m = jnp.max(s, axis=1, keepdims=True)
            weights = jnp.exp2((s - m) * scale).astype(bf16)
            acc = jnp.dot(weights, v_s[...], preferred_element_type=f32)
            out = (acc[:, :128] / acc[:, 128:]).astype(bf16)
            for i in range(block_rows // ROWS):
                p = n * (block_rows // ROWS) + i
                mine = out[ROWS * i:ROWS * (i + 1), :]
                if b < 2:
                    o_ref[p, ROWS * b:ROWS * (b + 1), :] = mine
                else:
                    o_ref[p, 56:64, :] = jnp.where(eight < 4, o_ref[p, 56:64, :], mine[56:])
                    o_ref[p, 120:128, :] = jnp.where(eight < 4, o_ref[p, 120:128, :], mine[:8])
                    o_ref[p, 128:PACK, :] = mine[8:24]
                    rest = mine[24:]
                    for k in range(3):
                        rows = slice(PIECE * k, PIECE * k + REST)
                        o_ref[p, rows, :] = jnp.where(rest_block == junk, turned(rest, 32 * (3 - k)), o_ref[p, rows, :])


def attend(seat, packed):
    return pl.pallas_call(
        attend_kernel,
        out_shape=jax.ShapeDtypeStruct((HEADS, PACK, 128), jnp.bfloat16),
        in_specs=[pl.BlockSpec(memory_space=pltpu.SMEM), pl.BlockSpec(memory_space=pltpu.VMEM)],
        out_specs=pl.BlockSpec(memory_space=pltpu.VMEM),
        scratch_shapes=[
            pltpu.VMEM((KEYS, 128), jnp.bfloat16),
            pltpu.VMEM((KEYS, 128), jnp.bfloat16),
            pltpu.VMEM((KEYS, 256), jnp.bfloat16),
            pltpu.VMEM((HEADS, TOKENS, 128), jnp.bfloat16),
            pltpu.VMEM((ROWS, HEADS * 128), jnp.float32),
        ],
        cost_estimate=pl.CostEstimate(flops=3 * 4 * KEYS * KEYS * 128, bytes_accessed=3 * 10**6, transcendentals=3 * KEYS * KEYS),
        compiler_params=pltpu.CompilerParams(vmem_limit_bytes=16 * 2**20),
        name="attend",
    )(seat, packed)


def project_kernel(x_ref, tokens_ref, weight_ref, o_ref, a_s):
    f32, bf16 = jnp.float32, jnp.bfloat16
    rest_block = lane_block(REST)

    def rest(h):
        first = (3 * h) % 4
        a, b, c = (turned(x_ref[h, PIECE * i:PIECE * i + REST, :], 32 * (i + 1)) for i in range(3))
        return jnp.where(rest_block == first, a, jnp.where(rest_block == (first + 1) % 4, b, c))

    a_s[TOKENS:, :] = jnp.zeros((a_s.shape[0] - TOKENS, D), bf16)
    for g in range(HEADS // 4):
        for part in range(4):
            size = PIECE if part < 3 else REST
            if part < 3:
                rows = [x_ref[4 * g + j, PIECE * part:PIECE * (part + 1), :] for j in range(4)]
            else:
                rows = [rest(4 * g + j) for j in range(4)]
            for i in range(3):
                lanes = slice(128 * (3 * g + i), 128 * (3 * g + i + 1))
                a_s[PIECE * part:PIECE * part + size, lanes] = jnp.where(
                    lane_block(size) < 3 - i, rows[i], rows[i + 1])
    for n in range(D // 512):
        cols = slice(512 * n, 512 * (n + 1))
        total = jnp.dot(a_s[...], weight_ref[:, cols], preferred_element_type=f32)
        for dst, src, count in SPANS:
            part = total[2 * dst:2 * (dst + count)].reshape(count, 2, 512)
            here = (slice(src, src + count), 0, slice(None), cols)
            o_ref[here] = (part + tokens_ref[here].astype(f32)).astype(bf16)


def project(returned, tokens, weight):
    vmem = pl.BlockSpec(memory_space=pltpu.VMEM)
    return pl.pallas_call(
        project_kernel,
        out_shape=jax.ShapeDtypeStruct(tokens.shape, jnp.bfloat16),
        in_specs=[vmem] * 3,
        out_specs=vmem,
        scratch_shapes=[pltpu.VMEM((192, D), jnp.bfloat16)],
        cost_estimate=pl.CostEstimate(flops=2 * 192 * D * D, bytes_accessed=7 * 10**6, transcendentals=0),
        compiler_params=pltpu.CompilerParams(vmem_limit_bytes=12 * 2**20),
        name="project",
    )(returned, tokens, weight)


def per_device(qkv_grid, tokens, out_weight, regions):
    windows, members = lax.axis_size("win"), lax.axis_size("seq")
    half = members // 2
    groups = [
        [w * members + half + i for i in range(half)] + [(w + 1) % windows * members + i for i in range(half)]
        for w in range(windows)
    ]

    def exchange(x):
        return lax.all_to_all(x, ("win", "seq"), 0, 0, axis_index_groups=groups, tiled=True)

    seat = lax.rem(lax.axis_index("seq") + half, members).reshape(1)
    received = exchange(pack_qkv(seat, qkv_grid, regions[:, 0].T))
    returned = exchange(attend(seat, received))
    return project(returned, tokens, out_weight)


def solution(mesh):
    in_specs = (P(None, "win", "seq", None), P(None, "win", "seq", None), P(), P(None, "win", None))
    out_specs = P(None, "win", "seq", None)
    return jax.shard_map(
        per_device, mesh=mesh, in_specs=in_specs, out_specs=out_specs, check_vma=False
    )
```

```python
import jax
import jax.numpy as jnp
from jax import lax
from jax.experimental import pallas as pl
from jax.experimental.pallas import tpu as pltpu
from jax.sharding import PartitionSpec as P

D = 1536
HEADS = 16
HD = 96
WH = 30
WW = 32
BANDS = 3
ROWS = 64
TOKENS = 184
SENT = 416
TAIL = 136
PACK = 136
REST = 44
KEYS = HEADS * ROWS
HIDE = -1e30


def lane_block(rows):
    return lax.broadcasted_iota(jnp.int32, (rows, 128), 1) // 32


def head_lanes(load, h):
    g, j = divmod(h, 4)
    if j == 0:
        return load(3 * g)
    if j == 3:
        return load(3 * g + 2)
    first, second = load(3 * g + j - 1), load(3 * g + j)
    block = lane_block(first.shape[0])
    return jnp.where(block < 3 - j, second, first)


def turned(x, shift):
    return pltpu.roll(x.astype(jnp.float32), shift, 1).astype(jnp.bfloat16)


SPANS = ((0, 15, 30), (30, 75, 2), (32, 45, 30), (62, 77, 13), (75, 0, 15))
SEGMENTS = ((0, 136, 0, 0, 0, 0), (136, 184, 0, 136, 1, 0), (184, 272, 1, 0, 1, 48), (272, 368, 1, 88, 2, 0), (368, 408, 2, 0, 2, 96))


def pack_kernel(seat_ref, x_ref, labels_ref, o_ref, flat):
    f32, bf16 = jnp.float32, jnp.bfloat16
    flat[TOKENS - 8:, :] = jnp.zeros((flat.shape[0] - TOKENS + 8, 3 * D), bf16)
    for dst, src, count in SPANS:
        for r in range(0, count, 8):
            n = min(8, count - r)
            start = 2 * (dst + r)
            flat[start:start + 2 * n, :] = x_ref[src + r:src + r + n, 0].reshape(2 * n, 3 * D)
    row = lax.broadcasted_iota(jnp.int32, (8, WW), 0)
    column = lax.rem(2 * seat_ref[0] + jnp.where(row < 3, 0, WW // 2), WW)
    picks = (lax.broadcasted_iota(jnp.int32, (8, WW), 1) == column).astype(bf16)
    picked = jnp.dot(picks, labels_ref[...], preferred_element_type=f32).astype(bf16)
    grid_row = lax.broadcasted_iota(jnp.int32, (90, 128), 0)
    lane = lax.broadcasted_iota(jnp.int32, (90, 128), 1) % 32
    band = lax.broadcasted_iota(jnp.int32, (8, 128), 0) % 3
    labels = jnp.zeros((8, 128), f32)
    for b in range(BANDS):
        place = ((grid_row == lane + WH * b) & (lane < WH)).astype(bf16)
        labels += jnp.where(band == b, jnp.dot(picked, place, preferred_element_type=f32), 0.0)
    labels = labels.astype(bf16)
    for h in range(HEADS):
        def rows(t, start, size):
            def load(tile):
                lanes = (12 * t + tile) * 128
                return flat[start:start + size, lanes:lanes + 128]
            return head_lanes(load, h)
        tail = rows(2, TOKENS - TAIL, TAIL)
        for start, end, t, first, section, skip in SEGMENTS:
            size = end - start
            moved = turned(tail[skip:skip + size], 32 * (3 - section))
            o_ref[h, start:end, :] = jnp.where(lane_block(size) == 3 - h % 4, moved, rows(t, first, size))
        o_ref[h, SENT - 8:, :] = jnp.where(lane_block(8) == 3 - h % 4, labels, rows(2, 40, 8))


def pack_qkv(seat, x, labels):
    vmem = pl.BlockSpec(memory_space=pltpu.VMEM)
    return pl.pallas_call(
        pack_kernel,
        out_shape=jax.ShapeDtypeStruct((HEADS, SENT, 128), jnp.bfloat16),
        in_specs=[pl.BlockSpec(memory_space=pltpu.SMEM), vmem, vmem],
        out_specs=vmem,
        scratch_shapes=[pltpu.VMEM((192, 3 * D), jnp.bfloat16)],
        cost_estimate=pl.CostEstimate(flops=10**7, bytes_accessed=4 * 10**6, transcendentals=0),
        compiler_params=pltpu.CompilerParams(vmem_limit_bytes=12 * 2**20),
        name="pack_qkv",
    )(seat, x, labels)


def attend_kernel(seat_ref, x_ref, o_ref, q_s, k_s, v_s, t_s, r_s):
    junk = 3 - lax.rem(seat_ref[0], 4)
    first = lax.rem(junk + 1, 4)
    second = lax.rem(junk + 2, 4)
    f32, bf16 = jnp.float32, jnp.bfloat16
    i32 = jnp.int32
    scale = HD ** -0.5 * 1.4426950408889634

    lane = lax.broadcasted_iota(i32, (ROWS, 128), 1) - 32 * junk
    inside = (lane >= 0) & (lane < 32)
    row = lax.broadcasted_iota(i32, (ROWS, 128), 0)
    sent_labels = jnp.concatenate([x_ref[p, SENT - 8:, :] for p in range(HEADS // 2)], 0)
    pick_row = lax.broadcasted_iota(i32, (ROWS, HEADS * 128), 0)
    pick_source = lax.broadcasted_iota(i32, (ROWS, HEADS * 128), 1) // 128
    pick_base = 8 * (pick_source % 8) + 3 * (pick_source // 8)
    tail_block = lane_block(TAIL)
    rest_block = lane_block(REST)
    eight = lax.broadcasted_iota(i32, (8, 128), 0)

    def block_of(load, b):
        if b < 2:
            return load(ROWS * b, ROWS)
        last = jnp.where(eight < 4, load(TOKENS - 8, 8), load(56, 8))
        return jnp.concatenate([load(120, 56), last], 0)

    def prepare(b):
        token = jnp.where(row < 60, row, row - 60) if b == 2 else row
        grows = (inside & (lane == token // 2)).astype(bf16)
        by_source = lax.dot_general(
            grows, sent_labels, (((1,), (1,)), ((), ())), preferred_element_type=f32).astype(bf16)
        picks = (pick_row == pick_base + b).astype(bf16)
        r_s[b % 2] = jnp.dot(by_source, picks, preferred_element_type=f32)

    def unpack(b, p):
        spare = (row < 4) if b == 2 else (row >= 60)
        label = jnp.where(spare, 3, r_s[b % 2, :, 128 * p:128 * (p + 1)].astype(i32))
        same = label == lane
        q = block_of(lambda start, size: x_ref[p, start:start + size, :], b)
        k = block_of(lambda start, size: x_ref[p, TOKENS + start:TOKENS + start + size, :], b)
        here = slice(ROWS * p, ROWS * (p + 1))
        q_s[b % 2, here, :] = jnp.where(inside, jnp.where(same, 1.0, 0.0).astype(bf16), q)
        k_s[b % 2, here, :] = jnp.where(inside, jnp.where(same, 0.0, HIDE).astype(bf16), k)
        if b == 0:
            x, y, z = (turned(x_ref[p, TAIL * i:TAIL * (i + 1), :], 32 * (i + 1)) for i in range(3))
            t_s[p, :TOKENS - TAIL, :] = x_ref[p, 2 * TOKENS:3 * TOKENS - TAIL, :]
            t_s[p, TOKENS - TAIL:, :] = jnp.where(tail_block == first, x, jnp.where(tail_block == second, y, z))
        v_s[b % 2, here, :128] = block_of(lambda start, size: t_s[p, start:start + size, :], b)

    v_s[:, :, 128:] = jnp.ones((2, KEYS, 128), bf16)
    prepare(0)
    for p in range(HEADS):
        unpack(0, p)
    for b in range(BANDS):
        if b + 1 < BANDS:
            prepare(b + 1)
        block_rows = 256
        for n in range(KEYS // block_rows):
            q = q_s[b % 2, block_rows * n:block_rows * (n + 1), :]
            s = lax.dot_general(q, k_s[b % 2], (((1,), (1,)), ((), ())), preferred_element_type=f32)
            if b + 1 < BANDS:
                for p in range(4 * n, 4 * n + 4):
                    unpack(b + 1, p)
            m = jnp.max(s, axis=1, keepdims=True)
            weights = jnp.exp2((s - m) * scale).astype(bf16)
            acc = jnp.dot(weights, v_s[b % 2], preferred_element_type=f32)
            out = (acc[:, :128] / acc[:, 128:]).astype(bf16)
            for i in range(block_rows // ROWS):
                p = n * (block_rows // ROWS) + i
                mine = out[ROWS * i:ROWS * (i + 1), :]
                if b < 2:
                    o_ref[p, ROWS * b:ROWS * (b + 1), :] = mine
                else:
                    o_ref[p, 56:64, :] = jnp.where(eight < 4, o_ref[p, 56:64, :], mine[56:])
                    o_ref[p, 120:128, :] = jnp.where(eight < 4, o_ref[p, 120:128, :], mine[:8])
                    o_ref[p, 128:PACK, :] = mine[8:16]
                    rest = mine[16:60]
                    for k in range(3):
                        rows = slice(REST * k, REST * (k + 1))
                        o_ref[p, rows, :] = jnp.where(rest_block == junk, turned(rest, 32 * (3 - k)), o_ref[p, rows, :])


def attend(seat, packed):
    return pl.pallas_call(
        attend_kernel,
        out_shape=jax.ShapeDtypeStruct((HEADS, PACK, 128), jnp.bfloat16),
        in_specs=[pl.BlockSpec(memory_space=pltpu.SMEM), pl.BlockSpec(memory_space=pltpu.VMEM)],
        out_specs=pl.BlockSpec(memory_space=pltpu.VMEM),
        scratch_shapes=[
            pltpu.VMEM((2, KEYS, 128), jnp.bfloat16),
            pltpu.VMEM((2, KEYS, 128), jnp.bfloat16),
            pltpu.VMEM((2, KEYS, 256), jnp.bfloat16),
            pltpu.VMEM((HEADS, TOKENS, 128), jnp.bfloat16),
            pltpu.VMEM((2, ROWS, HEADS * 128), jnp.float32),
        ],
        cost_estimate=pl.CostEstimate(flops=3 * 4 * KEYS * KEYS * 128, bytes_accessed=3 * 10**6, transcendentals=3 * KEYS * KEYS),
        compiler_params=pltpu.CompilerParams(vmem_limit_bytes=16 * 2**20),
        name="attend",
    )(seat, packed)


def project_kernel(x_ref, tokens_ref, weight_ref, o_ref, a_s):
    f32, bf16 = jnp.float32, jnp.bfloat16
    rest_block = lane_block(REST)

    def rest(h):
        first = (3 * h) % 4
        a, b, c = (turned(x_ref[h, REST * i:REST * (i + 1), :], 32 * (i + 1)) for i in range(3))
        return jnp.where(rest_block == first, a, jnp.where(rest_block == (first + 1) % 4, b, c))

    a_s[176:, :] = jnp.zeros((a_s.shape[0] - 176, D), bf16)
    for g in range(HEADS // 4):
        for start, end in ((0, 48), (48, 96), (96, PACK), (PACK, PACK + REST)):
            if start < PACK:
                rows = [x_ref[4 * g + j, start:end, :] for j in range(4)]
            else:
                rows = [rest(4 * g + j) for j in range(4)]
            for i in range(3):
                lanes = slice(128 * (3 * g + i), 128 * (3 * g + i + 1))
                a_s[start:end, lanes] = jnp.where(lane_block(end - start) < 3 - i, rows[i], rows[i + 1])
    for n in range(D // 512):
        cols = slice(512 * n, 512 * (n + 1))
        total = jnp.dot(a_s[...], weight_ref[:, cols], preferred_element_type=f32)
        for dst, src, count in SPANS:
            part = total[2 * dst:2 * (dst + count)].reshape(count, 2, 512)
            here = (slice(src, src + count), 0, slice(None), cols)
            o_ref[here] = (part + tokens_ref[here].astype(f32)).astype(bf16)


def project(returned, tokens, weight):
    vmem = pl.BlockSpec(memory_space=pltpu.VMEM)
    return pl.pallas_call(
        project_kernel,
        out_shape=jax.ShapeDtypeStruct(tokens.shape, jnp.bfloat16),
        in_specs=[vmem] * 3,
        out_specs=vmem,
        scratch_shapes=[pltpu.VMEM((192, D), jnp.bfloat16)],
        cost_estimate=pl.CostEstimate(flops=2 * 192 * D * D, bytes_accessed=7 * 10**6, transcendentals=0),
        compiler_params=pltpu.CompilerParams(vmem_limit_bytes=12 * 2**20),
        name="project",
    )(returned, tokens, weight)


def per_device(qkv_grid, tokens, out_weight, regions):
    windows, members = lax.axis_size("win"), lax.axis_size("seq")
    half = members // 2
    groups = [
        [w * members + half + i for i in range(half)] + [(w + 1) % windows * members + i for i in range(half)]
        for w in range(windows)
    ]

    def exchange(x):
        return lax.all_to_all(x, ("win", "seq"), 0, 0, axis_index_groups=groups, tiled=True)

    seat = lax.rem(lax.axis_index("seq") + half, members).reshape(1)
    received = exchange(pack_qkv(seat, qkv_grid, regions[:, 0].T.astype(jnp.bfloat16)))
    returned = exchange(attend(seat, received))
    return project(returned, tokens, out_weight)


def solution(mesh):
    in_specs = (P(None, "win", "seq", None), P(None, "win", "seq", None), P(), P(None, "win", None))
    out_specs = P(None, "win", "seq", None)
    return jax.shard_map(
        per_device, mesh=mesh, in_specs=in_specs, out_specs=out_specs, check_vma=False
    )
```
